256 devices in a mesh: row: 32 (over z_hi, y, x), col: 8 (over z_lo, core).
Axes of the slice: x: 4, y: 4, z: 8 (z_hi: 2, z_lo: 4; z = z_hi * 4 + z_lo), core: 2. Of those that a mesh axis runs over, the one named last changes fastest.
Arguments:
- w_integral: bfloat16 [38400, 4800], P('row', 'col'), may hold values from -0.125 to 0.125
- amplitudes: bfloat16 [4800, 4800], P('row', 'col'), may hold values from -6 to 6
- task_tiles: int32 [32, 7], P('row'), may hold values from -1 to 7, as said below
Outputs:
- residual: bfloat16 [38400, 4800], P('row', 'col')
The draws below stay inside these ranges and needn't reach their ends.
Inputs may be any that keep to these rules, and one draw needn't show every extreme that they name: `task_tiles`: in each row block the live entries come first, name distinct contraction tiles, and number 1 to 7; the remaining entries are -1. Some row block has 7 live entries, and row blocks 2 m and 2 m + 1 together have exactly 8.
All inputs are finite; a program needn't handle non-finite values.
Results may differ from the reference program's by a relative error of at most 0.001.
Values may be sent and summed in bfloat16 or wider, within the bound.
No kernel may reach another device: no remote copies, remote signals or barrier semaphores. Data moves between devices by JAX's collectives and lax.ppermute only.
A program may use at most 128 MiB of HBM per device.

```python
import jax
import jax.numpy as jnp

TILE = 24
OCC_BLK = 25
MOST = 7
PAIR = 8
KT = 8
KTS = 600
ROWS = 38400
KCON = 4800
COLS = 4800
ROW_BLOCKS = 32


def order_tiles(sub_key):
    return jax.random.permutation(sub_key, KT)


def draw_task_tiles(key, part):
    key_count, key_force, key_flip, key_order = jax.random.split(key, 4)
    pair_count = ROW_BLOCKS // 2
    leading = jax.random.randint(key_count, (pair_count,), PAIR - MOST, MOST + 1)
    forced = jax.random.randint(key_force, (), 0, pair_count)
    leading = jnp.where(jnp.arange(pair_count) == forced, MOST, leading)
    flipped = jax.random.randint(key_flip, (pair_count,), 0, 2)
    even_count = jnp.where(flipped == 1, PAIR - leading, leading)
    counts_all = jnp.stack([even_count, PAIR - even_count], axis=1).reshape(ROW_BLOCKS)
    orders = jax.vmap(order_tiles)(jax.random.split(key_order, ROW_BLOCKS))
    slot_index = jnp.arange(MOST)
    chosen = jnp.where(slot_index[None, :] < counts_all[:, None], orders[:, :MOST], -1)
    return chosen.astype(jnp.int32)


def levels(stream_key, dims, pieces, smallest, top_value):
    gain, own = 1.0, jax.random.fold_in(stream_key, 6)
    for dim, blocks in pieces:
        draws = jnp.exp(jax.random.uniform(jax.random.fold_in(own, dim), (blocks,), jnp.float32, smallest / len(pieces), top_value / len(pieces)))
        gain = gain * jnp.repeat(draws, dims[dim] // blocks).reshape([-1 if axis == dim else 1 for axis in range(len(dims))])
    return gain


def bell_draw(own_key, dims, spread, most, cuts=(), kind=jnp.bfloat16):
    factor_of = levels(own_key, dims, cuts, -0.22, 0.18) if cuts else 1.0
    result = jax.random.normal(own_key, dims, jnp.float32) * spread * factor_of
    return jnp.minimum(jnp.maximum(result, -most), most).astype(kind)


def setup_inputs(seed: int = 0) -> dict:
    seeds = jax.random.split(jax.random.key(seed), 4)
    return {
        "w_integral": bell_draw(seeds[0], (ROWS, KCON), (4 * KTS) ** -0.5, 0.125, ((0, 32), (1, 8))),
        "amplitudes": bell_draw(seeds[1], (KCON, COLS), 1.0, 6.0, ((0, 32), (1, 8))),
        "task_tiles": draw_task_tiles(jax.random.fold_in(seeds[3], 71), 0),
    }


def reference(w_integral, amplitudes, task_tiles):
    tile_ids = jnp.arange(KT, dtype=jnp.int32)
    live = jnp.sum((task_tiles[:, :, None] == tile_ids[None, None, :]).astype(jnp.int32), axis=1)
    block_rows = ROWS // ROW_BLOCKS
    tile_width = OCC_BLK * TILE
    shaped = w_integral.reshape(ROW_BLOCKS, block_rows, KT, tile_width)
    masked = shaped * live[:, None, :, None].astype(w_integral.dtype)
    cycle_term = jnp.dot(masked.reshape(ROWS, KCON), amplitudes, preferred_element_type=jnp.float32)
    return cycle_term.astype(jnp.bfloat16)
```

```python
import functools

import jax
import jax.numpy as jnp
from jax import lax
from jax.experimental import pallas as pl
from jax.experimental.pallas import tpu as pltpu
from jax.sharding import Mesh
from jax.sharding import PartitionSpec as P

ROW = ("zh", "y", "x")
COL = ("zl", "core")
UP = (None, ((0, 1), (1, 2), (2, 3)), ((1, 2), (2, 3)), ((2, 3),))
DOWN = (None, ((1, 0), (2, 1), (3, 2)), ((2, 1), (1, 0)), ((1, 0),))
SWAP = ((0, 1), (1, 0))
FROM = tuple(tuple((i, (i - n) % 4) for i in range(4)) for n in range(4))


def row_chunks(rows):
    cut = rows * 2 // 3
    return ((0, cut), (cut, rows))


def whole_tiles(pair):
    halves, depth, width = pair.shape
    by_distance = [pair] + [None] * 3
    for n in (1, 3, 2):
        by_distance[n] = lax.ppermute(pair, "x", FROM[n])

    def kernel(*refs):
        x = lax.axis_index("x")
        for place in range(4):

            @pl.when(x == place)
            def _():
                for half in range(halves):
                    shards = [
                        refs[(n - place) % 4][half].astype(jnp.float32)
                        for n in range(4)
                    ]
                    refs[4 + half][...] = jnp.concatenate(shards).astype(pair.dtype)

    inside = pl.BlockSpec(memory_space=pltpu.VMEM)
    return pl.pallas_call(
        kernel,
        out_shape=[jax.ShapeDtypeStruct((4 * depth, width), pair.dtype)] * halves,
        in_specs=[inside] * 4,
        out_specs=[inside] * halves,
    )(*by_distance)


def amplitude_tiles(amplitudes):
    other = lax.ppermute(amplitudes, "zh", SWAP)
    pair = jnp.stack([amplitudes, other])
    same_half, other_half = whole_tiles(pair)
    same_after = lax.ppermute(same_half, "y", FROM[1])
    same_before = lax.ppermute(same_half, "y", FROM[3])
    other_after = lax.ppermute(other_half, "y", FROM[1])
    other_before = lax.ppermute(other_half, "y", FROM[3])
    same_far, other_far = whole_tiles(lax.ppermute(pair, "y", FROM[2]))
    return [
        [same_half, same_after, same_far, same_before],
        [other_half, other_after, other_far, other_before],
    ]


LATE = ((1, 1), (1, 3))
EARLY = tuple((h, n) for h in range(2) for n in range(4) if (h, n) not in LATE)


def contract(origins, blocks, tiles, task_tiles, before, slots, place=None, out=None):
    pieces = [len(b) for b in blocks]
    wanted = sorted({key for _, _, keys in origins for key in keys})
    depth, width = tiles[0][0].shape
    rows = sum(p.shape[0] for p in blocks[0])
    last = place is not None
    anywhere = pl.BlockSpec(memory_space=pltpu.HBM)
    inside = pl.BlockSpec(memory_space=pltpu.VMEM)
    if last:
        out_shape = [jax.ShapeDtypeStruct((place[1], width), jnp.bfloat16)]
        out_specs = [anywhere]
    else:
        chunks = row_chunks(rows)
        out_shape = [jax.ShapeDtypeStruct((b - a, width), jnp.float32) for a, b in chunks]
        out_specs = [inside] * len(chunks)

    def kernel(task_ref, *refs):
        refs = list(refs)
        parts = [[refs.pop(0) for _ in range(n)] for n in pieces]
        tile_refs = {key: refs.pop(0) for key in wanted}
        before_refs = [refs.pop(0) for _ in before]
        if out is not None:
            refs.pop(0)
        out_refs = [refs.pop(0) for _ in out_shape]
        weights, columns, piece_sem, tile_sem, total = refs[:5]
        zl, core = lax.axis_index("zl"), lax.axis_index("core")
        zh, y = lax.axis_index("zh"), lax.axis_index("y")

        count = jnp.int32(0)
        for (away, swapped, keys), part in zip(origins, parts):
            source = zl + away
            tile = 2 * source + (1 - core if swapped else core)
            live = task_ref[0, 0] == tile
            for slot in range(1, task_tiles.shape[1]):
                live = live | (task_ref[0, slot] == tile)
            live = live & (source >= 0) & (source <= 3)
            inside_half = lax.rem(jnp.maximum(tile, 0), 4)
            half = (lax.div(tile, 4) != zh).astype(jnp.int32)
            y_distance = lax.rem(inside_half - y + 4, 4)
            if len(keys) < 8:
                listed = [(half == h) & (y_distance == n) for h, n in keys]
                live = live & functools.reduce(jnp.logical_or, listed)

            @pl.when(live)
            def _():
                first = 0
                for piece in part:
                    pltpu.make_async_copy(
                        piece,
                        weights.at[count, pl.ds(first, piece.shape[0])],
                        piece_sem.at[count],
                    ).start()
                    first += piece.shape[0]

            for h, n in keys:

                @pl.when(live & (half == h) & (y_distance == n))
                def _():
                    pltpu.make_async_copy(
                        tile_refs[h, n], columns.at[count], tile_sem.at[count]
                    ).start()

            count = count + live.astype(jnp.int32)

        if not before:
            total[...] = jnp.zeros_like(total)
        first = 0
        for before_ref in before_refs:
            total[pl.ds(first, before_ref.shape[0])] = before_ref[...]
            first += before_ref.shape[0]

        def step(n, carry):
            pltpu.make_async_copy(weights.at[n], weights.at[n], piece_sem.at[n]).wait()
            pltpu.make_async_copy(columns.at[n], columns.at[n], tile_sem.at[n]).wait()
            total[...] += jnp.dot(
                weights[n], columns[n], preferred_element_type=jnp.float32
            )
            return carry

        lax.fori_loop(0, count, step, 0)
        if last:
            rounded, out_sem = refs[5:]
            rounded[...] = total[...].astype(jnp.bfloat16)
            store = pltpu.make_async_copy(
                rounded, out_refs[0].at[pl.ds(place[0], rows)], out_sem
            )
            store.start()
            store.wait()
        else:
            for (a, b), out_ref in zip(chunks, out_refs):
                out_ref[...] = total[pl.ds(a, b - a)]

    arrays = [task_tiles] + [p for b in blocks for p in b]
    arrays += [tiles[h][n] for h, n in wanted]
    in_specs = [pl.BlockSpec(memory_space=pltpu.SMEM)] + [anywhere] * (len(arrays) - 1)
    scratch = [
        pltpu.VMEM((slots, rows, depth), jnp.bfloat16),
        pltpu.VMEM((slots, depth, width), jnp.bfloat16),
        pltpu.SemaphoreType.DMA((slots,)),
        pltpu.SemaphoreType.DMA((slots,)),
        pltpu.VMEM((rows, width), jnp.float32),
    ]
    aliases = {}
    arrays += before
    in_specs += [inside] * len(before)
    if last:
        scratch += [pltpu.VMEM((rows, width), jnp.bfloat16), pltpu.SemaphoreType.DMA(())]
    if out is not None:
        aliases = {len(arrays): 0}
        arrays.append(out)
        in_specs.append(anywhere)
    return pl.pallas_call(
        kernel,
        out_shape=out_shape,
        in_specs=in_specs,
        out_specs=out_specs,
        scratch_shapes=scratch,
        input_output_aliases=aliases,
        compiler_params=pltpu.CompilerParams(vmem_limit_bytes=48 * 1024 * 1024),
        cost_estimate=pl.CostEstimate(
            flops=2 * slots * rows * depth * width, bytes_accessed=0, transcendentals=0
        ),
    )(*arrays)


def everything(w_integral, amplitudes, task_tiles):
    rows = w_integral.shape[0]
    chunks = row_chunks(rows)
    here = {n: [] for n in range(-3, 4)}
    there = {n: [] for n in range(-3, 4)}
    here[0] = [w_integral]
    there[0] = [lax.ppermute(w_integral, "core", SWAP)]
    for a, b in chunks:
        up = down = w_integral[a:b]
        for n in (1, 2, 3):
            up = lax.ppermute(up, "zl", UP[n])
            down = lax.ppermute(down, "zl", DOWN[n])
            here[-n].append(up)
            here[n].append(down)
            there[-n].append(lax.ppermute(up, "core", SWAP))
            there[n].append(lax.ppermute(down, "core", SWAP))

    tiles = amplitude_tiles(amplitudes)

    def part(groups, piece, *more):
        origins = [(n, s, k) for d, k in groups for n in d for s in (False, True)]
        blocks = [(there if s else here)[n][piece] for n, s, _ in origins]
        return contract(origins, blocks, tiles, task_tiles, *more)

    every = EARLY + LATE
    sums = part([((0, -1, 1), EARLY)], slice(None), [], 6)
    sums = part([((0, -1, 1), LATE), ((-2, 2), every)], slice(None), list(sums), 4)
    out = None
    for k, (a, _) in enumerate(chunks):
        last = slice(k, k + 1), [sums[k]], 2, (a, rows)
        (out,) = part([((-3, 3), every)], *last, out)
    return out


def solution(mesh):
    torus = Mesh(mesh.devices.reshape(2, 4, 4, 4, 2), ROW + COL)
    return jax.shard_map(
        everything,
        mesh=torus,
        in_specs=(P(ROW, COL), P(ROW, COL), P(ROW, None)),
        out_specs=P(ROW, COL),
        check_vma=False,
    )
```
